32 devices in a mesh: grp: 8 (over z, x), sub: 4 (over y, core).
Axes of the slice: x: 2, y: 2, z: 4, core: 2. Of those that a mesh axis runs over, the one named last changes fastest.
Arguments:
- resid: bfloat16 [8, 4, 512, 512], P('grp', 'sub'), may hold values from -6 to 6
- neighbour_map: int32 [8, 4, 4], P('grp', 'sub'), may hold values from 0 to 3
- schur: bfloat16 [8, 4, 512, 512], P('grp', 'sub'), may hold values from -0.25 to 0.25
- deflation: bfloat16 [8, 4, 32, 512], P('grp', 'sub'), may hold values from -0.25 to 0.25
- forward_panels: bfloat16 [8, 128, 128], P('grp'), may hold values from -1 to 1
- block_inverses: bfloat16 [8, 128, 128], P('grp'), may hold values from -0.5 to 0.5
- scaling: float32 [8, 4, 512], P('grp', 'sub'), may hold values from 0.25 to 1
Outputs:
- applied: bfloat16 [8, 4, 512, 512], P('grp', 'sub')
The draws below stay inside these ranges and needn't reach their ends.
Inputs may be any that keep to these rules, and one draw needn't show every extreme that they name: `neighbour_map`: direction codes 0 to 3 as in the reference program.
All inputs are finite; a program needn't handle non-finite values.
Results may differ from the reference program's by a relative error of at most 0.013.
Values may be sent and summed in bfloat16 or wider, within the bound.
No kernel may reach another device: no remote copies, remote signals or barrier semaphores. Data moves between devices by JAX's collectives and lax.ppermute only.
A program may use at most 64 MiB of HBM per device.

```python
import math
import jax
import jax.numpy as jnp
from jax import lax

NI = 512
R = 512
C = 32
IFACE_BLOCK = 128
GROUPS = 8
MEMBERS = 4
KB = 128
NB = 4


def draw_forward_panels(key, part):
    first, second = jax.random.split(jax.random.fold_in(key, 11))
    normals = jax.random.normal(first, (GROUPS, KB, KB), jnp.float32)
    basis, unused = jnp.linalg.qr(normals)
    factor = jax.random.uniform(second, (GROUPS, 1, 1), jnp.float32, 0.9, 0.97)
    return (basis * factor).astype(jnp.bfloat16)


def plant(array, stream_key, smallest, high):
    index_at = [jax.random.randint(jax.random.fold_in(stream_key, axis), (), 0, length) for axis, length in enumerate(array.shape)]
    widest = array.shape.index(max(array.shape))
    beside = index_at[:widest] + [(index_at[widest] + 1) % array.shape[widest]] + index_at[widest + 1:]
    return array.at[tuple(index_at)].set(smallest).at[tuple(beside)].set(high)


def block_scale(own_key, shape, cuts, smallest, largest):
    loudness = 1.0
    for dim, shards_of in cuts:
        heights = jax.random.uniform(jax.random.fold_in(jax.random.fold_in(own_key, 6), dim), (shards_of,), jnp.float32, smallest / len(cuts), largest / len(cuts))
        loudness = loudness * jnp.repeat(jnp.exp(heights), shape[dim] // shards_of).reshape((-1,) + (1,) * (len(shape) - 1 - dim))
    return loudness


def gaussian(rng, extent, spread, bound, cuts=(), dtype=jnp.bfloat16):
    entries = jax.random.normal(rng, extent, jnp.float32) * spread
    if len(cuts) > 0:
        entries = block_scale(rng, extent, cuts, -0.22, 0.18) * entries
    return jnp.clip(entries, min=-bound, max=bound).astype(dtype)


def setup_inputs(seed: int = 0) -> dict:
    key_list = jax.random.split(jax.random.key(seed), 8)
    resid = gaussian(key_list[0], (GROUPS, MEMBERS, R, NI), 1.0, 6.0, ((0, 8), (1, 4)))
    neighbour_map = plant(jax.random.randint(key_list[1], (GROUPS, MEMBERS, NB), 0, 4), jax.random.fold_in(key_list[1], 1), 0, 3).astype(jnp.int32)
    schur = gaussian(key_list[2], (GROUPS, MEMBERS, NI, NI), NI ** -0.5, 0.25, ((0, 8), (1, 4)))
    deflation = gaussian(key_list[3], (GROUPS, MEMBERS, C, NI), NI ** -0.5, 0.25, ((0, 8), (1, 4)))
    forward_panels = draw_forward_panels(jax.random.fold_in(key_list[7], 71), 0)
    block_inverses = gaussian(key_list[5], (GROUPS, KB, KB), KB ** -0.5, 0.5, ((0, 8),))
    scaling = jnp.clip(jnp.exp(math.log(1.0) - 1.3862944 * jax.random.uniform(key_list[6], (GROUPS, MEMBERS, NI), jnp.float32) ** block_scale(key_list[6], (GROUPS, MEMBERS, NI), ((0, 8), (1, 4)), -0.2, 0.2)), 0.25, 1.0)
    return dict(resid=resid, neighbour_map=neighbour_map, schur=schur, deflation=deflation, forward_panels=forward_panels, block_inverses=block_inverses, scaling=scaling)


def assemble(field, neighbour_map):
    columns = jnp.repeat(neighbour_map, IFACE_BLOCK, axis=-1)[:, :, None, :]
    total = field.astype(jnp.float32)
    moves = ((1, 0), (-1, 0), (1, 1), (-1, 1))
    for code in range(4):
        moved = jnp.roll(field, moves[code][0], axis=moves[code][1]).astype(jnp.float32)
        total = total + jnp.where(columns == code, moved, jnp.float32(0.0))
    return total

def reference(resid, neighbour_map, schur, deflation, forward_panels, block_inverses, scaling):
    shared = assemble(resid, neighbour_map).astype(jnp.bfloat16)
    restricted = jnp.einsum('gmrn,gmcn->gmrc', shared.astype(jnp.float32), deflation.astype(jnp.float32), precision=lax.Precision.HIGHEST)
    coarse = jnp.transpose(restricted, (0, 2, 1, 3)).reshape(GROUPS, R, KB)

    def advance(previous, inputs):
        block, panel = inputs
        current = block + jnp.dot(previous, panel.astype(jnp.float32), precision=lax.Precision.HIGHEST)
        return (current, current)
    start = jnp.zeros((R, KB), jnp.float32)
    unused, carried = lax.scan(advance, start, (coarse, forward_panels))
    solved = jnp.einsum('grk,gkl->grl', carried, block_inverses.astype(jnp.float32), precision=lax.Precision.HIGHEST)
    lifted = jnp.transpose(solved.reshape(GROUPS, R, MEMBERS, C), (0, 2, 1, 3))

    def per_subdomain(inputs):
        lift_one, shared_one, defl_one, schur_one, scale_one = inputs
        correction = jnp.dot(lift_one, defl_one.astype(jnp.float32), precision=lax.Precision.HIGHEST)
        correction_low = correction.astype(jnp.bfloat16)
        before = jnp.dot(shared_one.astype(jnp.float32), schur_one.astype(jnp.float32), preferred_element_type=jnp.float32)
        after = jnp.dot(correction_low.astype(jnp.float32), schur_one.astype(jnp.float32), preferred_element_type=jnp.float32)
        return (correction + scale_one[None, :] * (before - after)).astype(jnp.bfloat16)
    count = GROUPS * MEMBERS
    local = lax.map(per_subdomain, (lifted.reshape(count, R, C), shared.reshape(count, R, NI), deflation.reshape(count, C, NI), schur.reshape(count, NI, NI), scaling.reshape(count, NI)))
    local = local.reshape(GROUPS, MEMBERS, R, NI)
    return assemble(local, neighbour_map).astype(jnp.bfloat16)
```

```python
import jax
import jax.numpy as jnp
from jax import lax
from jax.sharding import PartitionSpec as P


MOST_WEIGHTS = 1 << 20


def swap(block, axis, partner):
    return lax.ppermute(block, axis, [(i, partner(i)) for i in range(lax.axis_size(axis))])


def near(i):
    return i ^ 1


def far(size):
    return lambda i: (i + 1) % size if i % 2 else (i - 1) % size


def exchange(block):
    groups, members = lax.axis_size("grp"), lax.axis_size("sub")
    grp_far = swap(block, "grp", far(groups))
    sub_far = swap(block, "sub", far(members))
    grp_near = swap(block, "grp", near)
    sub_near = swap(block, "sub", near)
    return grp_near, grp_far, sub_near, sub_far


def chosen(neighbour_map):
    codes = neighbour_map[0, 0]
    even_g = lax.axis_index("grp") % 2 == 0
    even_m = lax.axis_index("sub") % 2 == 0
    before_g, after_g, before_m, after_m = (codes == code for code in range(4))
    return (
        jnp.where(even_g, after_g, before_g),
        jnp.where(even_g, before_g, after_g),
        jnp.where(even_m, after_m, before_m),
        jnp.where(even_m, before_m, after_m),
    )


def exact(left, right):
    return jnp.dot(left, right, precision=lax.Precision.HIGHEST)


def gather_pairs(block, axis):
    size = lax.axis_size(axis)
    stack = block[None]
    bit = 1
    while bit < size:
        stack = jnp.concatenate([stack, swap(stack, axis, lambda i: i ^ bit)])
        bit *= 2
    return stack


def coarse_weights(forward_panels, block_inverses, targets):
    groups = lax.axis_size("grp")
    here = lax.axis_index("grp")
    both = gather_pairs(jnp.concatenate([forward_panels, block_inverses]), "grp")
    order = jnp.bitwise_xor(jnp.arange(groups), here)
    both = both[order].astype(jnp.float32)
    panels, inverses = both[:, 0], both[:, 1]
    first = jnp.concatenate([inverses[t] for t in targets], axis=1)
    kb = panels.shape[-1]
    place = jnp.repeat(jnp.stack(targets), kb)[None, :]
    below = jnp.zeros_like(first)
    weights = [None] * groups
    for h in range(groups - 1, -1, -1):
        if h < groups - 1:
            below = exact(panels[h + 1], below)
        below = jnp.where(place == h, first, below)
        weights[h] = below
    return jnp.stack(weights)[order].astype(jnp.bfloat16)


def solved_by_weights(coarse, weights):
    coarse_all = gather_pairs(coarse, "grp")
    return lax.dot_general(
        weights, coarse_all, (((0, 1), (0, 1)), ((), ())), preferred_element_type=jnp.float32
    ).astype(jnp.bfloat16)


def solved_by_ring(coarse, panel, inverse):
    groups = lax.axis_size("grp")
    start = coarse.astype(jnp.float32)
    panel, inverse = panel.astype(jnp.float32).T, inverse.astype(jnp.float32).T

    def advance(step, state):
        received = lax.ppermute(state, "grp", [(i, i + 1) for i in range(groups - 1)])
        return start + exact(panel, received)

    carried = lax.fori_loop(0, groups - 1, advance, start)
    solved = exact(inverse, carried).astype(jnp.bfloat16)
    return jnp.concatenate([solved, swap(solved, "grp", near), swap(solved, "grp", far(groups))])


def body(resid, neighbour_map, schur, deflation, forward_panels, block_inverses, scaling):
    groups, members = lax.axis_size("grp"), lax.axis_size("sub")
    field, defl, local_schur, scale = resid[0, 0], deflation[0, 0], schur[0, 0], scaling[0]
    rows, columns = field.shape
    vectors = defl.shape[0]
    part = rows // members
    picks = chosen(neighbour_map)
    masks = [jnp.repeat(pick, columns // pick.shape[0])[None, :] for pick in picks]

    fields = exchange(field)
    here = lax.axis_index("grp")
    step = jnp.where(here % 2 == 0, 1, -1)
    targets = (here, (here + step) % groups, (here - step) % groups)
    gathered = groups * block_inverses.size * len(targets) <= MOST_WEIGHTS
    if gathered:
        weights = coarse_weights(forward_panels, block_inverses, targets)
    defl_schur = jnp.dot(defl, local_schur, preferred_element_type=jnp.float32)
    lift_basis = (defl.astype(jnp.float32) - scale * defl_schur).astype(jnp.bfloat16)

    total = field.astype(jnp.float32)
    for mask, moved in zip(masks, fields):
        total = total + jnp.where(mask, moved.astype(jnp.float32), 0.0)
    shared = total.astype(jnp.bfloat16)

    restricted = lax.dot_general(
        defl, shared, (((1,), (1,)), ((), ())), preferred_element_type=jnp.float32
    ).astype(jnp.bfloat16)
    restricted = restricted.reshape(vectors, members, part).transpose(1, 0, 2)
    coarse = lax.all_to_all(restricted, "sub", 0, 0).reshape(members * vectors, part)

    base = (scale * jnp.dot(shared, local_schur, preferred_element_type=jnp.float32)).astype(jnp.bfloat16)
    sent = jnp.concatenate([base, lift_basis])
    others = exchange(sent)

    if gathered:
        solved = solved_by_weights(coarse, weights)
    else:
        solved = solved_by_ring(coarse, forward_panels[0], block_inverses[0])
    solved = solved.reshape(3, members, vectors, part)
    sub_far = far(members)
    shares = jnp.stack(
        [
            jnp.concatenate(
                [solved[0, m], solved[1, m], solved[2, m], solved[0, near(m)], solved[0, sub_far(m)]]
            )
            for m in range(members)
        ]
    )
    lifted = lax.all_to_all(shares, "sub", 0, 0)

    basis = jnp.concatenate(
        [lift_basis] + [jnp.where(mask, other[rows:], 0) for mask, other in zip(masks, others)]
    )
    change = lax.dot_general(
        lifted, basis, (((1,), (0,)), ((), ())), preferred_element_type=jnp.float32
    ).reshape(rows, columns)
    total = change + base.astype(jnp.float32)
    for mask, other in zip(masks, others):
        total = total + jnp.where(mask, other[:rows].astype(jnp.float32), 0.0)
    return total.astype(jnp.bfloat16)[None, None]


def solution(mesh):
    return jax.shard_map(
        body,
        mesh=mesh,
        in_specs=(
            P("grp", "sub", None, None),
            P("grp", "sub", None),
            P("grp", "sub", None, None),
            P("grp", "sub", None, None),
            P("grp", None, None),
            P("grp", None, None),
            P("grp", "sub", None),
        ),
        out_specs=P("grp", "sub", None, None),
        check_vma=False,
    )
```

```python
import functools

import jax
import jax.numpy as jnp
from jax import lax
from jax.experimental import pallas as pl
from jax.experimental.pallas import tpu as pltpu
from jax.sharding import PartitionSpec as P


MOST_WEIGHTS = 1 << 20
CUTS_ONE = (4,)
CUTS_TWO = (3,)
VMEM = pl.BlockSpec(memory_space=pltpu.VMEM)
SMEM = pl.BlockSpec(memory_space=pltpu.SMEM)


def swap(block, axis, partner):
    route = [(i, partner(i)) for i in range(lax.axis_size(axis))]
    return lax.ppermute(block, axis, route)


def near(i):
    return i ^ 1


def far(size):
    return lambda i: (i + 1) % size if i % 2 else (i - 1) % size


def onward(size):
    return lambda i: (i + 2) % size if i % 2 == 0 else (i - 2) % size


def chunk_sizes(rows, eighths):
    ends = [rows * eighth // 8 for eighth in (0, *eighths, 8)]
    return [high - low for low, high in zip(ends, ends[1:])]


def chosen(neighbour_map):
    codes = neighbour_map[0, 0]
    odd_g, odd_m = lax.axis_index("grp") % 2, lax.axis_index("sub") % 2
    return jnp.where(codes < 2, (codes + 1 + odd_g) % 2, 2 + (codes + 1 + odd_m) % 2)


def exact(left, right):
    return jnp.dot(left, right, precision=lax.Precision.HIGHEST)


def bits_of(groups):
    bits, bit = [], 2
    while bit < groups:
        bits.append(bit)
        bit *= 2
    return [*bits, 1]


def weights_kernel(groups, vectors, place, stack, other, weights, below, picked):
    here, member = place[0], place[1]
    kb = stack.shape[3]
    targets = [place[2 + i] for i in range(weights.shape[0] // kb)]
    even, upper = member % 2 == 0, member // 2 % 2 == 0

    def slot(h):
        offset = h ^ here
        return sum(((offset // bit) % 2) << k for k, bit in enumerate(bits_of(groups)))

    def block(h, mine):
        own, twin = (jnp.where(mine, stack[i, slot(h)], other[i, slot(h)]) for i in range(2))
        return jnp.concatenate([jnp.where(upper, own, twin), jnp.where(upper, twin, own)])

    below[...] = jnp.zeros_like(below)
    for h in range(groups - 1, -1, -1):
        if h < groups - 1:
            value = below[...]
            high = value.astype(jnp.bfloat16)
            low = (value - high.astype(jnp.float32)).astype(jnp.bfloat16)
            left = block(h + 1, even)
            below[...] = jnp.dot(left, high, preferred_element_type=jnp.float32) + jnp.dot(
                left, low, preferred_element_type=jnp.float32
            )
        for i, target in enumerate(targets):

            @pl.when(target == h)
            def _():
                below[:, i * kb : (i + 1) * kb] = block(h, ~even).astype(jnp.float32)

        mine = below[pl.ds(pl.multiple_of(member * vectors, vectors), vectors)]
        picked[pl.ds(pl.multiple_of(slot(h) * vectors, vectors), vectors)] = mine
    weights[...] = picked[...].T.astype(jnp.bfloat16)


def coarse_weights(forward_panels, block_inverses, targets, vectors):
    groups, here, member = lax.axis_size("grp"), lax.axis_index("grp"), lax.axis_index("sub")
    kb = forward_panels.shape[-1]
    half = kb // 2
    kind = jnp.where(member % 2 == 0, forward_panels[0], block_inverses[0])
    stack = jnp.where(member // 2 % 2 == 0, kind[:half], kind[half:])[None]
    for bit in bits_of(groups):
        stack = jnp.concatenate([stack, swap(stack, "grp", lambda i: i ^ bit)])
    stack = jnp.stack([stack, swap(stack, "sub", lambda i: i ^ 2)])
    other = swap(stack, "sub", near)
    rows = len(targets) * kb
    return call(
        functools.partial(weights_kernel, groups, vectors),
        jax.ShapeDtypeStruct((rows, groups * vectors), jnp.bfloat16),
        [SMEM, VMEM, VMEM],
        [pltpu.VMEM((kb, rows), jnp.float32), pltpu.VMEM((groups * vectors, rows), jnp.float32)],
        4 * groups * kb * kb * rows,
        jnp.stack([here, member, *targets]).astype(jnp.int32), stack, other,
    )


def join_kernel(blocks, counts, pick, own, defl, *refs):
    *pieces, shared, restricted = refs
    width = own.shape[1] // blocks
    fields = [[pieces.pop(0) for _ in range(count)] for count in counts]
    for n in range(blocks):
        cols = slice(n * width, (n + 1) * width)
        for code, field in enumerate(fields):

            @pl.when(pick[n] == code)
            def _():
                row = 0
                for ref in field:
                    place = slice(row, row + ref.shape[0])
                    total = own[place, cols].astype(jnp.float32) + ref[:, cols].astype(jnp.float32)
                    shared[place, cols] = total.astype(jnp.bfloat16)
                    row += ref.shape[0]

    restricted[0] = lax.dot_general(
        defl[...], shared[...], (((1,), (1,)), ((), ())), preferred_element_type=jnp.float32
    ).astype(jnp.bfloat16)


def basis_kernel(defl, schur, scale, basis):
    defl_schur = jnp.dot(defl[...], schur[...], preferred_element_type=jnp.float32)
    basis[...] = (defl[...].astype(jnp.float32) - scale[...] * defl_schur).astype(jnp.bfloat16)


def base_kernel(shared, basis, schur, scale, whole, *chunks):
    vectors = basis.shape[0]
    base = jnp.dot(shared[...], schur[...], preferred_element_type=jnp.float32)
    base = (scale[...] * base).astype(jnp.bfloat16)
    whole[:vectors] = basis[...]
    whole[vectors:] = base
    chunks[0][:vectors] = basis[...]
    row = -vectors
    for chunk in chunks:
        skip = max(-row, 0)
        chunk[skip:] = base[row + skip : row + chunk.shape[0]]
        row += chunk.shape[0]


def share_sources(member, members):
    other = jnp.where(member % 2 == 0, member + members - 1, member + 1) % members
    return ((0, member), (1, member), (2, member), (0, member ^ 1), (0, other))


def solve_kernel(members, vectors, place, weights, *refs):
    *coarse, sent, kept, solved = refs
    me = place[1]
    kb = members * vectors
    total, slot = None, 0
    for ref in coarse:
        for j in range(ref.shape[0]):
            term = jnp.dot(
                weights[:, slot * vectors : (slot + 1) * vectors], ref[j], preferred_element_type=jnp.float32
            )
            total = term if total is None else total + term
            slot += 1
    solved[...] = total
    for j in range(members):
        share = kept if j % 2 == 0 else sent
        for i, (target, member) in enumerate(share_sources(me ^ j, members)):
            start = pl.multiple_of(target * kb + member * vectors, vectors)
            share[j // 2, i * vectors : (i + 1) * vectors] = solved[pl.ds(start, vectors)].astype(jnp.bfloat16)


def sum_kernel(blocks, counts, pick, whole, *refs):
    *pieces, total, basis = refs
    rows, columns = total.shape
    width, vectors = columns // blocks, whole.shape[0] - rows
    fields = [[pieces.pop(0) for _ in range(count)] for count in counts]
    basis[...] = jnp.zeros_like(basis)
    basis[:vectors] = whole[:vectors]
    for n in range(blocks):
        cols = slice(n * width, (n + 1) * width)
        for code, field in enumerate(fields):

            @pl.when(pick[n] == code)
            def _():
                basis[(code + 1) * vectors : (code + 2) * vectors, cols] = field[0][:vectors, cols]
                row = -vectors
                for ref in field:
                    skip = max(-row, 0)
                    place = slice(row + skip, row + ref.shape[0])
                    mine = whole[place.start + vectors : place.stop + vectors, cols].astype(jnp.float32)
                    total[place, cols] = mine + ref[skip:, cols].astype(jnp.float32)
                    row += ref.shape[0]


def last_kernel(total, basis, *refs):
    *lifted, out = refs
    left = lifted[0][...].astype(jnp.float32)
    for ref in lifted[1:]:
        left = left + ref[...].astype(jnp.float32)
    change = jnp.dot(left.astype(jnp.bfloat16).T, basis[...], preferred_element_type=jnp.float32)
    out[...] = (total[...] + change).astype(jnp.bfloat16)


def call(kernel, shapes, in_specs, scratch, cost, *args):
    single = not isinstance(shapes, (list, tuple))
    return pl.pallas_call(
        kernel,
        out_shape=shapes,
        in_specs=in_specs,
        out_specs=VMEM if single else [VMEM] * len(shapes),
        scratch_shapes=scratch,
        compiler_params=pltpu.CompilerParams(vmem_limit_bytes=12 << 20),
        cost_estimate=pl.CostEstimate(flops=cost, bytes_accessed=1 << 20, transcendentals=0),
    )(*args)


def solved_by_ring(coarse, panel, inverse):
    groups = lax.axis_size("grp")
    start = coarse.astype(jnp.float32)
    panel, inverse = panel.astype(jnp.float32).T, inverse.astype(jnp.float32).T

    def advance(step, state):
        received = lax.ppermute(state, "grp", [(i, i + 1) for i in range(groups - 1)])
        return start + exact(panel, received)

    carried = lax.fori_loop(0, groups - 1, advance, start)
    solved = exact(inverse, carried).astype(jnp.bfloat16)
    return jnp.concatenate([solved, swap(solved, "grp", near), swap(solved, "grp", far(groups))])


def lifted_by_ring(restricted, panel, inverse, members):
    vectors, rows = restricted.shape
    part = rows // members
    payload = restricted.reshape(vectors, members, part).transpose(1, 0, 2)
    coarse = lax.all_to_all(payload, "sub", 0, 0).reshape(members * vectors, part)
    solved = solved_by_ring(coarse, panel, inverse).reshape(3, members, vectors, part)
    sub_far = far(members)
    shares = jnp.stack(
        [
            jnp.concatenate([solved[0, m], solved[1, m], solved[2, m], solved[0, near(m)], solved[0, sub_far(m)]])
            for m in range(members)
        ]
    )
    return lax.all_to_all(shares, "sub", 0, 0).transpose(1, 0, 2).reshape(5 * vectors, rows)


def body(resid, neighbour_map, schur, deflation, forward_panels, block_inverses, scaling):
    groups, members = lax.axis_size("grp"), lax.axis_size("sub")
    field, defl, local_schur, scale = resid[0, 0], deflation[0, 0], schur[0, 0], scaling[0]
    rows, columns = field.shape
    vectors = defl.shape[0]
    blocks = neighbour_map.shape[-1]
    pick = chosen(neighbour_map)
    sub_far = far(members)
    bf16 = functools.partial(jax.ShapeDtypeStruct, dtype=jnp.bfloat16)

    near_g, low = [], 0
    for size in chunk_sizes(rows, CUTS_ONE):
        near_g.append(swap(field[low : low + size], "grp", near))
        low += size
    far_m = swap(field, "sub", sub_far)
    near_m = swap(field, "sub", near)
    far_g = [swap(piece, "grp", onward(groups)) for piece in near_g]

    here, member = lax.axis_index("grp"), lax.axis_index("sub")
    step = jnp.where(here % 2 == 0, 1, -1)
    targets = (here, (here + step) % groups, (here - step) % groups)
    gathered = groups * block_inverses.size * len(targets) <= MOST_WEIGHTS and groups & (groups - 1) == 0 and members == 4
    if gathered:
        weights = coarse_weights(forward_panels, block_inverses, targets, vectors)

    shared, restricted = call(
        functools.partial(join_kernel, blocks, (len(near_g), len(far_g), 1, 1)),
        [bf16((rows, columns)), bf16((1, vectors, rows))],
        [SMEM] + [VMEM] * (4 + len(near_g) + len(far_g)),
        [],
        2 * rows * columns * vectors,
        pick, field, defl, *near_g, *far_g, near_m, far_m,
    )
    basis = call(
        basis_kernel,
        bf16((vectors, columns)),
        [VMEM] * 3,
        [],
        2 * vectors * columns * columns,
        defl, local_schur, scale,
    )
    sizes = chunk_sizes(rows, CUTS_TWO)
    sizes[0] += vectors
    whole, *chunks = call(
        base_kernel,
        [bf16((vectors + rows, columns))] + [bf16((size, columns)) for size in sizes],
        [VMEM] * 4,
        [],
        2 * rows * columns * columns,
        shared, basis, local_schur, scale,
    )
    two_near_g = [swap(chunk, "grp", near) for chunk in chunks]
    two_far_g = [swap(chunk, "grp", onward(groups)) for chunk in two_near_g]
    two_near_m = swap(whole, "sub", near)
    two_far_m = swap(whole, "sub", sub_far)

    if gathered:
        pieces = [restricted]
        for bit in bits_of(groups):
            stack = jnp.concatenate(pieces) if len(pieces) > 1 else restricted
            pieces.append(swap(stack, "grp", lambda i: i ^ bit))
        half = (members // 2, 5 * vectors, rows)
        sent, kept = call(
            functools.partial(solve_kernel, members, vectors),
            [bf16(half), bf16(half)],
            [SMEM] + [VMEM] * (1 + len(pieces)),
            [pltpu.VMEM((weights.shape[0], rows), jnp.float32)],
            2 * weights.size * rows,
            jnp.stack([here, member]).astype(jnp.int32), weights, *pieces,
        )
        came = swap(sent, "sub", near)
        passed = (kept[1].astype(jnp.float32) + came[1].astype(jnp.float32)).astype(jnp.bfloat16)
        lifted = [kept[0], came[0], swap(passed, "sub", lambda i: i ^ 2)]
    else:
        lifted = [lifted_by_ring(restricted[0], forward_panels[0], block_inverses[0], members)]

    total, masked = call(
        functools.partial(sum_kernel, blocks, (len(two_near_g), len(two_far_g), 1, 1)),
        [jax.ShapeDtypeStruct((rows, columns), jnp.float32), bf16((5 * vectors, columns))],
        [SMEM] + [VMEM] * (3 + len(two_near_g) + len(two_far_g)),
        [],
        rows * columns,
        pick, whole, *two_near_g, *two_far_g, two_near_m, two_far_m,
    )
    out = call(
        last_kernel,
        bf16((rows, columns)),
        [VMEM] * (2 + len(lifted)),
        [],
        10 * vectors * rows * columns,
        total, masked, *lifted,
    )
    return out[None, None]


def solution(mesh):
    return jax.shard_map(
        body,
        mesh=mesh,
        in_specs=(
            P("grp", "sub", None, None),
            P("grp", "sub", None),
            P("grp", "sub", None, None),
            P("grp", "sub", None, None),
            P("grp", None, None),
            P("grp", None, None),
            P("grp", "sub", None),
        ),
        out_specs=P("grp", "sub", None, None),
        check_vma=False,
    )
```

```python
import functools

import jax
import jax.numpy as jnp
from jax import lax
from jax.experimental import pallas as pl
from jax.experimental.pallas import tpu as pltpu
from jax.sharding import PartitionSpec as P


MOST_WEIGHTS = 1 << 20
CUTS_ONE = (4,)
CUTS_TWO = (4,)
VMEM = pl.BlockSpec(memory_space=pltpu.VMEM)
SMEM = pl.BlockSpec(memory_space=pltpu.SMEM)


def swap(block, axis, partner):
    route = [(i, partner(i)) for i in range(lax.axis_size(axis))]
    return lax.ppermute(block, axis, route)


def near(i):
    return i ^ 1


def far(size):
    return lambda i: (i + 1) % size if i % 2 else (i - 1) % size


def onward(size):
    return lambda i: (i + 2) % size if i % 2 == 0 else (i - 2) % size


def chunk_sizes(rows, eighths):
    ends = [rows * eighth // 8 for eighth in (0, *eighths, 8)]
    return [high - low for low, high in zip(ends, ends[1:])]


def chosen(codes, n):
    odd_g, odd_m = lax.rem(lax.axis_index("grp"), 2), lax.rem(lax.axis_index("sub"), 2)
    code = codes[n]
    return jnp.where(code < 2, lax.rem(code + 1 + odd_g, 2), 2 + lax.rem(code + 1 + odd_m, 2))


def exact(left, right):
    return jnp.dot(left, right, precision=lax.Precision.HIGHEST)


def gathered_slot(offset, groups):
    return offset // 2 + offset % 2 * (groups // 2)


def share_sources(member, members):
    other = lax.rem(jnp.where(lax.rem(member, 2) == 0, member + members - 1, member + 1), members)
    return ((0, member), (1, member), (2, member), (0, member ^ 1), (0, other))


def kind_kernel(panel, inverse, kind):
    kind[...] = jnp.where(lax.rem(lax.axis_index("sub"), 2) == 0, panel[...], inverse[...])


def weights_kernel(groups, members, vectors, stack, other, weights, below, picked, turned):
    here, me = lax.axis_index("grp"), lax.axis_index("sub")
    kb = members * vectors
    step = 1 - 2 * lax.rem(here, 2)
    targets = [here, here + step, lax.rem(here - step + groups, groups)]
    even = lax.rem(me, 2) == 0

    def block(h, mine):
        slot = gathered_slot(h ^ here, groups)
        return jnp.where(mine, stack[slot], other[slot])

    below[...] = jnp.zeros_like(below)
    for h in range(groups - 1, -1, -1):
        if h < groups - 1:
            value = below[...]
            high = value.astype(jnp.bfloat16)
            low = (value - high.astype(jnp.float32)).astype(jnp.bfloat16)
            left = block(h + 1, even)
            below[...] = jnp.dot(left, high, preferred_element_type=jnp.float32) + jnp.dot(
                left, low, preferred_element_type=jnp.float32
            )
        for i, target in enumerate(targets):

            @pl.when(target == h)
            def _():
                below[:, i * kb : (i + 1) * kb] = block(h, ~even).astype(jnp.float32)

        slot = gathered_slot(h ^ here, groups)
        mine = below[pl.ds(pl.multiple_of(me * vectors, vectors), vectors)]
        picked[pl.ds(pl.multiple_of(slot * vectors, vectors), vectors)] = mine
    turned[...] = picked[...].T
    for j in range(members):
        for i, (target, member) in enumerate(share_sources(me ^ j, members)):
            start = pl.multiple_of(target * kb + member * vectors, vectors)
            weights[j, i * vectors : (i + 1) * vectors] = turned[pl.ds(start, vectors)].astype(jnp.bfloat16)


def coarse_weights(forward_panels, block_inverses, vectors):
    groups, members = lax.axis_size("grp"), lax.axis_size("sub")
    shape = jax.ShapeDtypeStruct(forward_panels.shape, forward_panels.dtype)
    stack = call(kind_kernel, shape, [VMEM] * 2, [], forward_panels.size, forward_panels, block_inverses)
    bits, bit = [], 2
    while bit < groups:
        bits.append(bit)
        bit *= 2
    for bit in (*bits, 1):
        came = swap(stack, "grp", lambda i: i ^ bit)
        stack = jnp.concatenate([stack, came])
    other = swap(stack, "sub", near)
    kb = stack.shape[2]
    width = groups * vectors
    return call(
        functools.partial(weights_kernel, groups, members, vectors),
        jax.ShapeDtypeStruct((members, 5 * vectors, width), jnp.bfloat16),
        [VMEM, VMEM],
        [
            pltpu.VMEM((kb, 3 * kb), jnp.float32),
            pltpu.VMEM((width, 3 * kb), jnp.float32),
            pltpu.VMEM((3 * kb, width), jnp.float32),
        ],
        12 * groups * kb * kb * kb,
        stack, other,
    )


def join_kernel(blocks, counts, codes, own, defl, *refs):
    *pieces, shared, restricted = refs
    width = own.shape[1] // blocks
    fields = [[pieces.pop(0) for _ in range(count)] for count in counts]
    for n in range(blocks):
        cols = slice(n * width, (n + 1) * width)
        for code, field in enumerate(fields):

            @pl.when(chosen(codes, n) == code)
            def _():
                row = 0
                for ref in field:
                    place = slice(row, row + ref.shape[0])
                    total = own[place, cols].astype(jnp.float32) + ref[:, cols].astype(jnp.float32)
                    shared[place, cols] = total.astype(jnp.bfloat16)
                    row += ref.shape[0]

    restricted[0] = lax.dot_general(
        defl[...], shared[...], (((1,), (1,)), ((), ())), preferred_element_type=jnp.float32
    ).astype(jnp.bfloat16)


def basis_kernel(defl, schur, scale, basis):
    defl_schur = jnp.dot(defl[...], schur[...], preferred_element_type=jnp.float32)
    basis[...] = (defl[...].astype(jnp.float32) - scale[...] * defl_schur).astype(jnp.bfloat16)


def base_kernel(shared, basis, schur, scale, whole, *chunks):
    vectors = basis.shape[0]
    base = jnp.dot(shared[...], schur[...], preferred_element_type=jnp.float32)
    base = (scale[...] * base).astype(jnp.bfloat16)
    whole[:vectors] = basis[...]
    whole[vectors:] = base
    chunks[0][:vectors] = basis[...]
    row = -vectors
    for chunk in chunks:
        skip = max(-row, 0)
        chunk[skip:] = base[row + skip : row + chunk.shape[0]]
        row += chunk.shape[0]


def solve_kernel(weights, *refs):
    *coarse, sent, kept = refs
    blocks = [ref[j] for ref in coarse for j in range(ref.shape[0])]
    coarse_all = jnp.concatenate(blocks)
    for j in range(weights.shape[0]):
        share = jnp.dot(weights[j], coarse_all, preferred_element_type=jnp.float32)
        (kept if j % 2 == 0 else sent)[j // 2] = share.astype(jnp.bfloat16)


def sum_kernel(blocks, counts, codes, whole, *refs):
    *pieces, total, basis = refs
    rows, columns = total.shape
    width, vectors = columns // blocks, whole.shape[0] - rows
    fields = [[pieces.pop(0) for _ in range(count)] for count in counts]
    basis[...] = jnp.zeros_like(basis)
    basis[:vectors] = whole[:vectors]
    for n in range(blocks):
        cols = slice(n * width, (n + 1) * width)
        for code, field in enumerate(fields):

            @pl.when(chosen(codes, n) == code)
            def _():
                basis[(code + 1) * vectors : (code + 2) * vectors, cols] = field[0][:vectors, cols]
                row = -vectors
                for ref in field:
                    skip = max(-row, 0)
                    place = slice(row + skip, row + ref.shape[0])
                    mine = whole[place.start + vectors : place.stop + vectors, cols].astype(jnp.float32)
                    total[place, cols] = mine + ref[skip:, cols].astype(jnp.float32)
                    row += ref.shape[0]


def last_kernel(total, basis, *refs):
    *lifted, out = refs
    left = lifted[0][...].astype(jnp.float32)
    for ref in lifted[1:]:
        left = left + ref[...].astype(jnp.float32)
    change = jnp.dot(left.astype(jnp.bfloat16).T, basis[...], preferred_element_type=jnp.float32)
    out[...] = (total[...] + change).astype(jnp.bfloat16)


def call(kernel, shapes, in_specs, scratch, cost, *args):
    single = not isinstance(shapes, (list, tuple))
    return pl.pallas_call(
        kernel,
        out_shape=shapes,
        in_specs=in_specs,
        out_specs=VMEM if single else [VMEM] * len(shapes),
        scratch_shapes=scratch,
        compiler_params=pltpu.CompilerParams(vmem_limit_bytes=10 << 20),
        cost_estimate=pl.CostEstimate(flops=cost, bytes_accessed=1 << 20, transcendentals=0),
    )(*args)


def solved_by_ring(coarse, panel, inverse):
    groups = lax.axis_size("grp")
    start = coarse.astype(jnp.float32)
    panel, inverse = panel.astype(jnp.float32).T, inverse.astype(jnp.float32).T

    def advance(step, state):
        received = lax.ppermute(state, "grp", [(i, i + 1) for i in range(groups - 1)])
        return start + exact(panel, received)

    carried = lax.fori_loop(0, groups - 1, advance, start)
    solved = exact(inverse, carried).astype(jnp.bfloat16)
    return jnp.concatenate([solved, swap(solved, "grp", near), swap(solved, "grp", far(groups))])


def lifted_by_ring(restricted, panel, inverse, members):
    vectors, rows = restricted.shape
    part = rows // members
    payload = restricted.reshape(vectors, members, part).transpose(1, 0, 2)
    coarse = lax.all_to_all(payload, "sub", 0, 0).reshape(members * vectors, part)
    solved = solved_by_ring(coarse, panel, inverse).reshape(3, members, vectors, part)
    sub_far = far(members)
    shares = jnp.stack(
        [
            jnp.concatenate([solved[0, m], solved[1, m], solved[2, m], solved[0, near(m)], solved[0, sub_far(m)]])
            for m in range(members)
        ]
    )
    return lax.all_to_all(shares, "sub", 0, 0).transpose(1, 0, 2).reshape(5 * vectors, rows)


def body(resid, neighbour_map, schur, deflation, forward_panels, block_inverses, scaling):
    groups, members = lax.axis_size("grp"), lax.axis_size("sub")
    field, defl, local_schur, scale = resid[0, 0], deflation[0, 0], schur[0, 0], scaling[0]
    rows, columns = field.shape
    vectors = defl.shape[0]
    blocks = neighbour_map.shape[-1]
    codes = neighbour_map[0, 0]
    sub_far = far(members)
    bf16 = functools.partial(jax.ShapeDtypeStruct, dtype=jnp.bfloat16)

    near_g, low = [], 0
    for size in chunk_sizes(rows, CUTS_ONE):
        near_g.append(swap(field[low : low + size], "grp", near))
        low += size
    far_m = swap(field, "sub", sub_far)
    near_m = swap(field, "sub", near)
    far_g = [swap(piece, "grp", onward(groups)) for piece in near_g]

    gathered = groups * block_inverses.size * 3 <= MOST_WEIGHTS and groups & (groups - 1) == 0 and members == 4
    if gathered:
        weights = coarse_weights(forward_panels, block_inverses, vectors)

    shared, restricted = call(
        functools.partial(join_kernel, blocks, (len(near_g), len(far_g), 1, 1)),
        [bf16((rows, columns)), bf16((1, vectors, rows))],
        [SMEM] + [VMEM] * (4 + len(near_g) + len(far_g)),
        [],
        2 * rows * columns * vectors,
        codes, field, defl, *near_g, *far_g, near_m, far_m,
    )
    basis = call(
        basis_kernel,
        bf16((vectors, columns)),
        [VMEM] * 3,
        [],
        2 * vectors * columns * columns,
        defl, local_schur, scale,
    )
    sizes = chunk_sizes(rows, CUTS_TWO)
    sizes[0] += vectors
    whole, *chunks = call(
        base_kernel,
        [bf16((vectors + rows, columns))] + [bf16((size, columns)) for size in sizes],
        [VMEM] * 4,
        [],
        2 * rows * columns * columns,
        shared, basis, local_schur, scale,
    )
    two_near_g = [swap(chunk, "grp", near) for chunk in chunks]
    two_far_g = [swap(chunk, "grp", onward(groups)) for chunk in two_near_g]
    two_near_m = swap(whole, "sub", near)
    two_far_m = swap(whole, "sub", sub_far)

    if gathered:
        pieces = [restricted]
        for offset in range(2, groups, 2):
            pieces.append(swap(restricted, "grp", lambda i: i ^ offset))
        stack = jnp.concatenate(pieces)
        half = (members // 2, 5 * vectors, rows)
        sent, kept = call(
            solve_kernel,
            [bf16(half), bf16(half)],
            [VMEM] * 3,
            [],
            2 * weights.size * rows,
            weights, stack, swap(stack, "grp", near),
        )
        came = swap(sent, "sub", near)
        passed = (kept[1].astype(jnp.float32) + came[1].astype(jnp.float32)).astype(jnp.bfloat16)
        lifted = [kept[0], came[0], swap(passed, "sub", lambda i: i ^ 2)]
    else:
        lifted = [lifted_by_ring(restricted[0], forward_panels[0], block_inverses[0], members)]

    total, masked = call(
        functools.partial(sum_kernel, blocks, (len(two_near_g), len(two_far_g), 1, 1)),
        [jax.ShapeDtypeStruct((rows, columns), jnp.float32), bf16((5 * vectors, columns))],
        [SMEM] + [VMEM] * (3 + len(two_near_g) + len(two_far_g)),
        [],
        rows * columns,
        codes, whole, *two_near_g, *two_far_g, two_near_m, two_far_m,
    )
    out = call(
        last_kernel,
        bf16((rows, columns)),
        [VMEM] * (2 + len(lifted)),
        [],
        10 * vectors * rows * columns,
        total, masked, *lifted,
    )
    return out[None, None]


def solution(mesh):
    return jax.shard_map(
        body,
        mesh=mesh,
        in_specs=(
            P("grp", "sub", None, None),
            P("grp", "sub", None),
            P("grp", "sub", None, None),
            P("grp", "sub", None, None),
            P("grp", None, None),
            P("grp", None, None),
            P("grp", "sub", None),
        ),
        out_specs=P("grp", "sub", None, None),
        check_vma=False,
    )
```

```python
import functools

import jax
import jax.numpy as jnp
from jax import lax
from jax.experimental import pallas as pl
from jax.experimental.pallas import tpu as pltpu
from jax.sharding import PartitionSpec as P


MOST_WEIGHTS = 1 << 20
CUTS_ONE = (4,)
VMEM = pl.BlockSpec(memory_space=pltpu.VMEM)
SMEM = pl.BlockSpec(memory_space=pltpu.SMEM)


def swap(block, axis, partner):
    route = [(i, partner(i)) for i in range(lax.axis_size(axis))]
    return lax.ppermute(block, axis, route)


def near(i):
    return i ^ 1


def far(size):
    return lambda i: (i + 1) % size if i % 2 else (i - 1) % size


def onward(size):
    return lambda i: (i + 2) % size if i % 2 == 0 else (i - 2) % size


def chunk_sizes(rows, eighths):
    ends = [rows * eighth // 8 for eighth in (0, *eighths, 8)]
    return [high - low for low, high in zip(ends, ends[1:])]


def chosen(codes, n):
    odd_g, odd_m = lax.rem(lax.axis_index("grp"), 2), lax.rem(lax.axis_index("sub"), 2)
    code = codes[n]
    return jnp.where(code < 2, lax.rem(code + 1 + odd_g, 2), 2 + lax.rem(code + 1 + odd_m, 2))


def exact(left, right):
    return jnp.dot(left, right, precision=lax.Precision.HIGHEST)


def gathered_slot(offset, groups):
    return offset // 2 + offset % 2 * (groups // 2)


def share_sources(member, members):
    other = lax.rem(jnp.where(lax.rem(member, 2) == 0, member + members - 1, member + 1), members)
    return ((0, member), (1, member), (2, member), (0, member ^ 1), (0, other))


def kind_kernel(panel, inverse, kind):
    kind[...] = jnp.where(lax.rem(lax.axis_index("sub"), 2) == 0, panel[...], inverse[...])


def weights_kernel(groups, members, vectors, stack, other, weights, below, picked, turned):
    here, me = lax.axis_index("grp"), lax.axis_index("sub")
    kb = members * vectors
    step = 1 - 2 * lax.rem(here, 2)
    targets = [here, here + step, lax.rem(here - step + groups, groups)]
    even = lax.rem(me, 2) == 0

    def block(h, mine):
        slot = gathered_slot(h ^ here, groups)
        return jnp.where(mine, stack[slot], other[slot])

    below[...] = jnp.zeros_like(below)
    for h in range(groups - 1, -1, -1):
        if h < groups - 1:
            value = below[...]
            high = value.astype(jnp.bfloat16)
            low = (value - high.astype(jnp.float32)).astype(jnp.bfloat16)
            left = block(h + 1, even)
            below[...] = jnp.dot(left, high, preferred_element_type=jnp.float32) + jnp.dot(
                left, low, preferred_element_type=jnp.float32
            )
        for i, target in enumerate(targets):

            @pl.when(target == h)
            def _():
                below[:, i * kb : (i + 1) * kb] = block(h, ~even).astype(jnp.float32)

        slot = gathered_slot(h ^ here, groups)
        mine = below[pl.ds(pl.multiple_of(me * vectors, vectors), vectors)]
        picked[pl.ds(pl.multiple_of(slot * vectors, vectors), vectors)] = mine
    turned[...] = picked[...].T
    for j in range(members):
        for i, (target, member) in enumerate(share_sources(me ^ j, members)):
            start = pl.multiple_of(target * kb + member * vectors, vectors)
            weights[j, i * vectors : (i + 1) * vectors] = turned[pl.ds(start, vectors)].astype(jnp.bfloat16)


def coarse_weights(forward_panels, block_inverses, vectors):
    groups, members = lax.axis_size("grp"), lax.axis_size("sub")
    shape = jax.ShapeDtypeStruct(forward_panels.shape, forward_panels.dtype)
    stack = call(kind_kernel, shape, [VMEM] * 2, [], forward_panels.size, forward_panels, block_inverses)
    bits, bit = [], 2
    while bit < groups:
        bits.append(bit)
        bit *= 2
    for bit in (*bits, 1):
        came = swap(stack, "grp", lambda i: i ^ bit)
        stack = jnp.concatenate([stack, came])
    other = swap(stack, "sub", near)
    kb = stack.shape[2]
    width = groups * vectors
    return call(
        functools.partial(weights_kernel, groups, members, vectors),
        jax.ShapeDtypeStruct((members, 5 * vectors, width), jnp.bfloat16),
        [VMEM, VMEM],
        [
            pltpu.VMEM((kb, 3 * kb), jnp.float32),
            pltpu.VMEM((width, 3 * kb), jnp.float32),
            pltpu.VMEM((3 * kb, width), jnp.float32),
        ],
        12 * groups * kb * kb * kb,
        stack, other,
    )


def join_kernel(blocks, low, codes, own, defl, near_g, far_g, near_m, far_m, *refs):
    *before, shared, restricted = refs
    size, columns = shared.shape
    width = columns // blocks
    rows = slice(low, low + size)
    for n in range(blocks):
        cols = slice(n * width, (n + 1) * width)
        for code, (ref, place) in enumerate(((near_g, slice(0, size)), (far_g, slice(0, size)), (near_m, rows), (far_m, rows))):

            @pl.when(chosen(codes, n) == code)
            def _():
                total = own[rows, cols].astype(jnp.float32) + ref[place, cols].astype(jnp.float32)
                shared[:, cols] = total.astype(jnp.bfloat16)

    for ref in before:
        restricted[0, :, :low] = ref[0]
    restricted[0, :, rows] = lax.dot_general(
        defl[...], shared[...], (((1,), (1,)), ((), ())), preferred_element_type=jnp.float32
    ).astype(jnp.bfloat16)


def basis_kernel(defl, schur, scale, basis):
    defl_schur = jnp.dot(defl[...], schur[...], preferred_element_type=jnp.float32)
    basis[...] = (defl[...].astype(jnp.float32) - scale[...] * defl_schur).astype(jnp.bfloat16)


def base_kernel(shared, basis, schur, scale, *refs):
    *before, chunk = refs[:-1] if len(refs) > 1 else refs
    base = jnp.dot(shared[...], schur[...], preferred_element_type=jnp.float32)
    base = (scale[...] * base).astype(jnp.bfloat16)
    skip = chunk.shape[0] - base.shape[0]
    if skip:
        chunk[:skip] = basis[...]
    chunk[skip:] = base
    if before:
        whole, row = refs[-1], 0
        for ref in before:
            whole[row : row + ref.shape[0]] = ref[...]
            row += ref.shape[0]
        whole[row:] = base


def solve_kernel(weights, *refs):
    *coarse, sent, kept = refs
    blocks = [ref[j] for ref in coarse for j in range(ref.shape[0])]
    coarse_all = jnp.concatenate(blocks)
    for j in range(weights.shape[0]):
        share = jnp.dot(weights[j], coarse_all, preferred_element_type=jnp.float32)
        (kept if j % 2 == 0 else sent)[j // 2] = share.astype(jnp.bfloat16)


def sum_kernel(blocks, counts, codes, whole, *refs):
    *pieces, total, basis = refs
    rows, columns = total.shape
    width, vectors = columns // blocks, whole.shape[0] - rows
    fields = [[pieces.pop(0) for _ in range(count)] for count in counts]
    basis[...] = jnp.zeros_like(basis)
    basis[:vectors] = whole[:vectors]
    for n in range(blocks):
        cols = slice(n * width, (n + 1) * width)
        for code, field in enumerate(fields):

            @pl.when(chosen(codes, n) == code)
            def _():
                basis[(code + 1) * vectors : (code + 2) * vectors, cols] = field[0][:vectors, cols]
                row = -vectors
                for ref in field:
                    skip = max(-row, 0)
                    place = slice(row + skip, row + ref.shape[0])
                    mine = whole[place.start + vectors : place.stop + vectors, cols].astype(jnp.float32)
                    total[place, cols] = mine + ref[skip:, cols].astype(jnp.float32)
                    row += ref.shape[0]


def last_kernel(total, basis, *refs):
    *lifted, out = refs
    left = lifted[0][...].astype(jnp.float32)
    for ref in lifted[1:]:
        left = left + ref[...].astype(jnp.float32)
    change = jnp.dot(left.astype(jnp.bfloat16).T, basis[...], preferred_element_type=jnp.float32)
    out[...] = (total[...] + change).astype(jnp.bfloat16)


def call(kernel, shapes, in_specs, scratch, cost, *args):
    single = not isinstance(shapes, (list, tuple))
    return pl.pallas_call(
        kernel,
        out_shape=shapes,
        in_specs=in_specs,
        out_specs=VMEM if single else [VMEM] * len(shapes),
        scratch_shapes=scratch,
        compiler_params=pltpu.CompilerParams(vmem_limit_bytes=10 << 20),
        cost_estimate=pl.CostEstimate(flops=cost, bytes_accessed=1 << 20, transcendentals=0),
    )(*args)


def solved_by_ring(coarse, panel, inverse):
    groups = lax.axis_size("grp")
    start = coarse.astype(jnp.float32)
    panel, inverse = panel.astype(jnp.float32).T, inverse.astype(jnp.float32).T

    def advance(step, state):
        received = lax.ppermute(state, "grp", [(i, i + 1) for i in range(groups - 1)])
        return start + exact(panel, received)

    carried = lax.fori_loop(0, groups - 1, advance, start)
    solved = exact(inverse, carried).astype(jnp.bfloat16)
    return jnp.concatenate([solved, swap(solved, "grp", near), swap(solved, "grp", far(groups))])


def lifted_by_ring(restricted, panel, inverse, members):
    vectors, rows = restricted.shape
    part = rows // members
    payload = restricted.reshape(vectors, members, part).transpose(1, 0, 2)
    coarse = lax.all_to_all(payload, "sub", 0, 0).reshape(members * vectors, part)
    solved = solved_by_ring(coarse, panel, inverse).reshape(3, members, vectors, part)
    sub_far = far(members)
    shares = jnp.stack(
        [
            jnp.concatenate([solved[0, m], solved[1, m], solved[2, m], solved[0, near(m)], solved[0, sub_far(m)]])
            for m in range(members)
        ]
    )
    return lax.all_to_all(shares, "sub", 0, 0).transpose(1, 0, 2).reshape(5 * vectors, rows)


def body(resid, neighbour_map, schur, deflation, forward_panels, block_inverses, scaling):
    groups, members = lax.axis_size("grp"), lax.axis_size("sub")
    field, defl, local_schur, scale = resid[0, 0], deflation[0, 0], schur[0, 0], scaling[0]
    rows, columns = field.shape
    vectors = defl.shape[0]
    blocks = neighbour_map.shape[-1]
    codes = neighbour_map[0, 0]
    sub_far = far(members)
    bf16 = functools.partial(jax.ShapeDtypeStruct, dtype=jnp.bfloat16)

    near_g, low = [], 0
    for size in chunk_sizes(rows, CUTS_ONE):
        near_g.append(swap(field[low : low + size], "grp", near))
        low += size
    far_m = swap(field, "sub", sub_far)
    near_m = swap(field, "sub", near)
    far_g = [swap(piece, "grp", onward(groups)) for piece in near_g]

    gathered = groups * block_inverses.size * 3 <= MOST_WEIGHTS and groups & (groups - 1) == 0 and members == 4
    if gathered:
        weights = coarse_weights(forward_panels, block_inverses, vectors)

    basis = call(
        basis_kernel,
        bf16((vectors, columns)),
        [VMEM] * 3,
        [],
        2 * vectors * columns * columns,
        defl, local_schur, scale,
    )
    low, before, chunks = 0, [], []
    sizes = chunk_sizes(rows, CUTS_ONE)
    for i, size in enumerate(sizes):
        shared, restricted = call(
            functools.partial(join_kernel, blocks, low),
            [bf16((size, columns)), bf16((1, vectors, low + size))],
            [SMEM] + [VMEM] * (6 + len(before)),
            [],
            2 * size * columns * vectors,
            codes, field, defl, near_g[i], far_g[i], near_m, far_m, *before,
        )
        last = i == len(sizes) - 1
        shapes = [bf16((size + (0 if i else vectors), columns))] + [bf16((vectors + rows, columns))] * last
        chunk, *whole = call(
            base_kernel,
            shapes,
            [VMEM] * (4 + len(chunks) * last),
            [],
            2 * size * columns * columns,
            shared, basis, local_schur, scale, *(chunks if last else []),
        )
        low, before, chunks = low + size, [restricted], [*chunks, chunk]
    whole = whole[0]
    two_near_g = [swap(chunk, "grp", near) for chunk in chunks]
    two_far_g = [swap(chunk, "grp", onward(groups)) for chunk in two_near_g]
    two_near_m = swap(whole, "sub", near)
    two_far_m = swap(whole, "sub", sub_far)

    if gathered:
        pieces = [restricted]
        for offset in range(2, groups, 2):
            pieces.append(swap(restricted, "grp", lambda i: i ^ offset))
        stack = jnp.concatenate(pieces)
        half = (members // 2, 5 * vectors, rows)
        sent, kept = call(
            solve_kernel,
            [bf16(half), bf16(half)],
            [VMEM] * 3,
            [],
            2 * weights.size * rows,
            weights, stack, swap(stack, "grp", near),
        )
        came = swap(sent, "sub", near)
        passed = (kept[1].astype(jnp.float32) + came[1].astype(jnp.float32)).astype(jnp.bfloat16)
        lifted = [kept[0], came[0], swap(passed, "sub", lambda i: i ^ 2)]
    else:
        lifted = [lifted_by_ring(restricted[0], forward_panels[0], block_inverses[0], members)]

    total, masked = call(
        functools.partial(sum_kernel, blocks, (len(two_near_g), len(two_far_g), 1, 1)),
        [jax.ShapeDtypeStruct((rows, columns), jnp.float32), bf16((5 * vectors, columns))],
        [SMEM] + [VMEM] * (3 + len(two_near_g) + len(two_far_g)),
        [],
        rows * columns,
        codes, whole, *two_near_g, *two_far_g, two_near_m, two_far_m,
    )
    out = call(
        last_kernel,
        bf16((rows, columns)),
        [VMEM] * (2 + len(lifted)),
        [],
        10 * vectors * rows * columns,
        total, masked, *lifted,
    )
    return out[None, None]


def solution(mesh):
    return jax.shard_map(
        body,
        mesh=mesh,
        in_specs=(
            P("grp", "sub", None, None),
            P("grp", "sub", None),
            P("grp", "sub", None, None),
            P("grp", "sub", None, None),
            P("grp", None, None),
            P("grp", None, None),
            P("grp", "sub", None),
        ),
        out_specs=P("grp", "sub", None, None),
        check_vma=False,
    )
```
